64 devices in a mesh: dp: 4 (over x, y), tp: 16 (over z, core).
Axes of the slice: x: 2, y: 2, z: 8, core: 2. Of those that a mesh axis runs over, the one named last changes fastest.
The devices are a block of a 4x4x8 slice.
Arguments:
- x_tokens: bfloat16 [4, 4096, 1536], P('dp', 'tp'), parts along dimension 0
- ln1_gain: float32 [2, 1536], replicated
- ln1_bias: float32 [2, 1536], replicated
- ln2_gain: float32 [2, 1536], replicated
- ln2_bias: float32 [2, 1536], replicated
- w_qkv: bfloat16 [2, 1536, 3, 16, 96], P(None, None, None, 'tp')
- w_out: bfloat16 [2, 16, 96, 1536], P(None, 'tp')
- b_out: float32 [2, 1536], replicated
- w_up: bfloat16 [2, 1536, 6144], P(None, None, 'tp')
- b_up: float32 [2, 6144], P(None, 'tp')
- w_down: bfloat16 [2, 6144, 1536], P(None, 'tp')
- b_down: float32 [2, 1536], replicated
Outputs:
- output: bfloat16 [4, 4096, 1536], P('dp', 'tp'), parts along dimension 0
There are 4 independent parts. The reference program is written for one: setup_inputs(seed, part) draws one part's arguments, and reference() takes and returns one part's arrays. A program takes and returns all parts, laid end to end along the dimension named above; an argument that names none is the same for every part.
All inputs are finite; a program needn't handle non-finite values.
Results may differ from the reference program's by a relative error of at most 0.010894.
Values are sent between devices in bfloat16 or wider.
A program may use at most 768 MiB of HBM per device.

```python
import math
import jax
import jax.numpy as jnp
from jax import lax

BATCH = 1
SEQ_LEN = 4096
D_MODEL = 1536
HEADS = 16
HEAD_DIM = 96
D_FF = 6144
LAYERS = 2


def setup_inputs(seed: int = 0, part: int = 0) -> dict:
    base_key = jax.random.key(seed)
    part_key = jax.random.fold_in(base_key, part)
    row_key, tok_key = jax.random.split(part_key)
    keys = jax.random.split(base_key, 11)
    row_scale = 0.5 + jax.random.uniform(row_key, (BATCH, SEQ_LEN, 1), jnp.float32)
    tokens = jax.random.normal(tok_key, (BATCH, SEQ_LEN, D_MODEL), jnp.float32) * row_scale
    qk_gain = (math.log(SEQ_LEN) / 2.0) ** 0.25
    attn_level = math.sqrt((1.0 + 0.5 * math.log(SEQ_LEN)) / math.sqrt(SEQ_LEN))
    out_gain = 0.5 / attn_level
    proj_gain = jnp.array([qk_gain, qk_gain, 1.0], jnp.float32).reshape(1, 1, 3, 1, 1)
    vec_shape = (LAYERS, D_MODEL)
    w_qkv = jax.random.normal(keys[4], (LAYERS, D_MODEL, 3, HEADS, HEAD_DIM), jnp.float32) * proj_gain * D_MODEL ** -0.5
    w_out = jax.random.normal(keys[5], (LAYERS, HEADS, HEAD_DIM, D_MODEL), jnp.float32) * (out_gain * D_MODEL ** -0.5)
    w_up = jax.random.normal(keys[7], (LAYERS, D_MODEL, D_FF), jnp.float32) * D_MODEL ** -0.5
    w_down = jax.random.normal(keys[9], (LAYERS, D_FF, D_MODEL), jnp.float32) * (0.8 * D_FF ** -0.5)
    return {
        "x_tokens": tokens.astype(jnp.bfloat16),
        "ln1_gain": 1.0 + 0.2 * jax.random.normal(keys[0], vec_shape, jnp.float32),
        "ln1_bias": 0.2 * jax.random.normal(keys[1], vec_shape, jnp.float32),
        "ln2_gain": 1.0 + 0.2 * jax.random.normal(keys[2], vec_shape, jnp.float32),
        "ln2_bias": 0.2 * jax.random.normal(keys[3], vec_shape, jnp.float32),
        "w_qkv": w_qkv.astype(jnp.bfloat16),
        "w_out": w_out.astype(jnp.bfloat16),
        "b_out": 0.2 * jax.random.normal(keys[6], vec_shape, jnp.float32),
        "w_up": w_up.astype(jnp.bfloat16),
        "b_up": 0.3 * jax.random.normal(keys[8], (LAYERS, D_FF), jnp.float32),
        "w_down": w_down.astype(jnp.bfloat16),
        "b_down": 0.2 * jax.random.normal(keys[10], vec_shape, jnp.float32),
    }


def layer_norm(resid, gain, shift):
    row_mean = jnp.mean(resid, axis=-1, keepdims=True)
    centered = resid - row_mean
    variance = jnp.mean(centered * centered, axis=-1, keepdims=True)
    return (centered * lax.rsqrt(variance + 1e-5) * gain + shift).astype(jnp.bfloat16)


def attention_head(head_parts):
    queries, keys_all, values_all = head_parts
    scores = jnp.einsum("bqe,bke->bqk", queries.astype(jnp.float32), keys_all.astype(jnp.float32)) / math.sqrt(HEAD_DIM)
    positions = jnp.arange(SEQ_LEN)
    causal = positions[:, None] >= positions[None, :]
    scores = jnp.where(causal, scores, -1e30)
    attn_probs = jax.nn.softmax(scores, axis=-1).astype(jnp.bfloat16)
    return jnp.einsum("bqk,bke->bqe", attn_probs.astype(jnp.float32), values_all.astype(jnp.float32)).astype(jnp.bfloat16)


def layer_step(resid, params):
    ln1_gain, ln1_bias, ln2_gain, ln2_bias, w_qkv, w_out, b_out, w_up, b_up, w_down, b_down = params
    normed = layer_norm(resid, ln1_gain, ln1_bias)
    qkv_proj = jnp.dot(normed.reshape(BATCH * SEQ_LEN, D_MODEL), w_qkv.reshape(D_MODEL, 3 * HEADS * HEAD_DIM), preferred_element_type=jnp.float32).astype(jnp.bfloat16)
    qkv_proj = qkv_proj.reshape(BATCH, SEQ_LEN, 3, HEADS, HEAD_DIM)
    heads_first = jnp.transpose(qkv_proj, (2, 3, 0, 1, 4))
    attn_heads = lax.map(attention_head, (heads_first[0], heads_first[1], heads_first[2]))
    attn_out = jnp.einsum("hbse,hed->bsd", attn_heads.astype(jnp.float32), w_out.astype(jnp.float32))
    resid = resid + (attn_out + b_out)
    normed_mlp = layer_norm(resid, ln2_gain, ln2_bias)
    pre_act = jnp.dot(normed_mlp.reshape(BATCH * SEQ_LEN, D_MODEL), w_up, preferred_element_type=jnp.float32) + b_up
    hidden = jax.nn.gelu(pre_act, approximate=True).astype(jnp.bfloat16)
    mlp_out = jnp.dot(hidden, w_down, preferred_element_type=jnp.float32).reshape(BATCH, SEQ_LEN, D_MODEL)
    resid = resid + (mlp_out + b_down)
    return resid, None


def reference(x_tokens, ln1_gain, ln1_bias, ln2_gain, ln2_bias, w_qkv, w_out, b_out, w_up, b_up, w_down, b_down):
    params = (ln1_gain, ln1_bias, ln2_gain, ln2_bias, w_qkv, w_out, b_out, w_up, b_up, w_down, b_down)
    resid, _ = lax.scan(layer_step, x_tokens.astype(jnp.float32), params)
    return resid.astype(jnp.bfloat16)
```

```python
import functools
import math
import jax
import jax.numpy as jnp
from jax import lax
from jax.experimental import pallas as pl
from jax.experimental.pallas import tpu as pltpu
from jax.sharding import PartitionSpec as P

BF16, F32 = jnp.bfloat16, jnp.float32
LANES = 128


def layer_norm(resid, gain, shift):
    row_mean = jnp.mean(resid, axis=-1, keepdims=True)
    centered = resid - row_mean
    variance = jnp.mean(centered * centered, axis=-1, keepdims=True)
    return (centered * lax.rsqrt(variance + 1e-5) * gain + shift).astype(BF16)


def attention_kernel(scale, share, head_dim, h_ref, w_ref, o_ref, k_scr, v_scr):
    i = pl.program_id(0)
    rows = h_ref.shape[0]
    qkv = jnp.dot(h_ref[...], w_ref[...], preferred_element_type=F32).astype(BF16)
    here = pl.ds(pl.multiple_of(i * rows, rows), rows)
    q, k, v = (qkv[:, n * LANES : (n + 1) * LANES] for n in range(3))
    k_scr[here, :] = k
    v_scr[here, :] = v
    to_exp2 = scale * math.log2(math.e)
    parts = rows // share
    queries = [q[n * share : (n + 1) * share] for n in range(parts)]

    def scores(keys, query):
        return lax.dot_general(keys, query, (((1,), (1,)), ((), ())), preferred_element_type=F32) * to_exp2

    def weighted(values, probs):
        return lax.dot_general(values, probs, (((0,), (0,)), ((), ())), preferred_element_type=F32)

    state = []
    for n in range(parts):
        s = scores(k, queries[n])
        key_at = lax.broadcasted_iota(jnp.int32, s.shape, 0)
        query_at = lax.broadcasted_iota(jnp.int32, s.shape, 1) + n * share
        s = jnp.where(key_at <= query_at, s, -1e30)
        top = jnp.max(s, axis=0, keepdims=True)
        p = jnp.exp2(s - top)
        state.append((top, jnp.sum(p, axis=0, keepdims=True), weighted(v, p.astype(BF16))))

    def step(j, state):
        there = pl.ds(pl.multiple_of(j * rows, rows), rows)
        keys, values = k_scr[there, :], v_scr[there, :]
        out = []
        for n, (top, total, acc) in enumerate(state):
            s = scores(keys, queries[n])
            new_top = jnp.maximum(top, jnp.max(s, axis=0, keepdims=True))
            shrink = jnp.exp2(top - new_top)
            p = jnp.exp2(s - new_top)
            total = total * shrink + jnp.sum(p, axis=0, keepdims=True)
            out.append((new_top, total, acc * shrink + weighted(values, p.astype(BF16))))
        return tuple(out)

    state = lax.fori_loop(0, i, step, tuple(state))
    for n, (_, total, acc) in enumerate(state):
        o_ref[n] = (acc / total)[:head_dim].astype(BF16)


def attention(gathered, w_head, share, head_dim):
    tokens, width = gathered.shape
    rows = 2 * share
    return pl.pallas_call(
        functools.partial(attention_kernel, 1.0 / math.sqrt(head_dim), share, head_dim),
        grid=(tokens // rows,),
        out_shape=jax.ShapeDtypeStruct((tokens // share, head_dim, share), BF16),
        in_specs=[pl.BlockSpec((rows, width), lambda i: (i, 0)), pl.BlockSpec((width, 3 * LANES), lambda i: (0, 0))],
        out_specs=pl.BlockSpec((rows // share, head_dim, share), lambda i: (i, 0, 0)),
        scratch_shapes=[pltpu.VMEM((tokens, LANES), BF16), pltpu.VMEM((tokens, LANES), BF16)],
        cost_estimate=pl.CostEstimate(flops=30_000_000_000, bytes_accessed=16_000_000, transcendentals=9_000_000),
        compiler_params=pltpu.CompilerParams(dimension_semantics=("arbitrary",), vmem_limit_bytes=32 * 1024 * 1024),
        name="attention",
    )(gathered, w_head)


def solution(mesh):
    tp_size, dp_size = mesh.shape["tp"], mesh.shape["dp"]
    bits = [1 << n for n in range(dp_size.bit_length() - 1)]

    def spread(block, order):
        held = {0: block}
        for bit in order:
            pairs = [(d, d ^ bit) for d in range(dp_size)]
            held.update({off ^ bit: lax.ppermute(b, "dp", pairs) for off, b in list(held.items())})
        return held

    def partner(x):
        return lax.ppermute(x, "tp", [(t, t ^ 1) for t in range(tp_size)])

    def local_forward(x_local, ln1_gain, ln1_bias, ln2_gain, ln2_bias, w_qkv, w_out, b_out, w_up, b_up, w_down, b_down):
        layers, width, hidden = w_up.shape
        share, head_dim = x_local.shape[1], w_out.shape[2]
        mine = lax.axis_index("dp")
        core = lax.rem(lax.axis_index("tp"), 2)
        part = hidden // dp_size

        def of_my_core(x):
            x = x.reshape(tp_size // 2, 2, *x.shape[1:])
            return lax.dynamic_index_in_dim(x, core, 1, keepdims=False)

        b_up_all = of_my_core(lax.all_gather(b_up, "tp", axis=0)).reshape(tp_size // 2, layers, dp_size, part)

        def mlp_weights(layer):
            up = lax.dynamic_slice_in_dim(w_up[layer], mine * part, part, 1).T
            down = lax.dynamic_slice_in_dim(w_down[layer], mine * part, part, 0)
            up = of_my_core(lax.all_gather(up, "tp", axis=0)).reshape(-1, width)
            down = of_my_core(lax.all_gather(down, "tp", axis=0)).reshape(-1, width)
            ups, downs = spread(up, bits), spread(down, bits[::-1])
            out = []
            for off in range(dp_size):
                bias = lax.dynamic_index_in_dim(b_up_all[:, layer], mine ^ off, 1, keepdims=False).reshape(-1)
                out.append((ups[off], bias, downs[off]))
            return out

        weights = [mlp_weights(layer) for layer in range(layers)]
        resid = x_local[0].astype(F32)
        for layer in range(layers):
            w_head = jnp.pad(w_qkv[layer][:, :, 0], ((0, 0), (0, 0), (0, LANES - head_dim))).reshape(width, 3 * LANES)
            normed = layer_norm(resid, ln1_gain[layer], ln1_bias[layer])
            gathered = lax.all_gather(normed, "tp", axis=0, tiled=True)
            heads = attention(gathered, w_head, share, head_dim)
            heads = lax.all_to_all(heads, "tp", 0, 0, tiled=True).reshape(-1, share)
            w_out_all = lax.all_gather(w_out[layer][0], "tp", axis=0, tiled=True)
            attn = lax.dot_general(heads, w_out_all, (((0,), (0,)), ((), ())), preferred_element_type=F32)
            resid = resid + (attn + b_out[layer])
            normed_mlp = layer_norm(resid, ln2_gain[layer], ln2_bias[layer])
            both = jnp.concatenate([normed_mlp, partner(normed_mlp)], 0)
            total = None
            for up, bias, down in weights[layer]:
                pre_act = lax.dot_general(both, up, (((1,), (1,)), ((), ())), preferred_element_type=F32) + bias
                act = jax.nn.gelu(pre_act, approximate=True).astype(BF16)
                term = jnp.dot(act, down, preferred_element_type=F32)
                total = term if total is None else total + term
            mlp = total[:share] + partner(total[share:])
            resid = resid + (mlp + b_down[layer])
        return resid.astype(BF16)[None]

    rows_spec = P("dp", "tp", None)
    in_specs = (rows_spec, P(), P(), P(), P(), P(None, None, None, "tp", None), P(None, "tp", None, None), P(), P(None, None, "tp"), P(None, "tp"), P(None, "tp", None), P())
    return jax.shard_map(local_forward, mesh=mesh, in_specs=in_specs, out_specs=rows_spec, check_vma=False)
```

```python
import functools
import math
import jax
import jax.numpy as jnp
from jax import lax
from jax.experimental import pallas as pl
from jax.experimental.pallas import tpu as pltpu
from jax.sharding import PartitionSpec as P

BF16, F32 = jnp.bfloat16, jnp.float32
LANES = 128


def layer_norm(resid, gain, shift):
    row_mean = jnp.mean(resid, axis=-1, keepdims=True)
    centered = resid - row_mean
    variance = jnp.mean(centered * centered, axis=-1, keepdims=True)
    return (centered * lax.rsqrt(variance + 1e-5) * gain + shift).astype(BF16)


def attention_kernel(scale, part, share, head_dim, h_ref, w_ref, o_ref, k_scr, v_scr):
    i = pl.program_id(0)
    rows = k_scr.shape[0] // pl.num_programs(0)
    here = pl.ds(pl.multiple_of(i * rows, rows), rows)
    hidden = h_ref[...].reshape(rows, h_ref.shape[-1])
    qkv = jnp.dot(hidden, w_ref[...], preferred_element_type=F32).astype(BF16)
    q, k, v = (qkv[:, n * LANES : (n + 1) * LANES] for n in range(3))
    k_scr[here, :] = k
    v_scr[here, :] = v
    to_exp2 = scale * math.log2(math.e)
    queries = [q[n * part : (n + 1) * part] for n in range(rows // part)]

    def scores(keys, query):
        return lax.dot_general(keys, query, (((1,), (1,)), ((), ())), preferred_element_type=F32) * to_exp2

    def weighted(values, probs):
        return lax.dot_general(values, probs, (((0,), (0,)), ((), ())), preferred_element_type=F32)

    state = []
    for n, query in enumerate(queries):
        seen = (n + 1) * part
        s = scores(k[:seen], query)
        key_at = lax.broadcasted_iota(jnp.int32, s.shape, 0)
        query_at = lax.broadcasted_iota(jnp.int32, s.shape, 1) + n * part
        s = jnp.where(key_at <= query_at, s, -1e30)
        top = jnp.max(s, axis=0, keepdims=True)
        p = jnp.exp2(s - top)
        state.append((top, jnp.sum(p, axis=0, keepdims=True), weighted(v[:seen], p.astype(BF16))))

    def step(j, state):
        there = pl.ds(pl.multiple_of(j * rows, rows), rows)
        keys, values = k_scr[there, :], v_scr[there, :]
        blocks = [scores(keys, query) for query in queries]
        out = []
        for s, (top, total, acc) in zip(blocks, state):
            new_top = jnp.maximum(top, jnp.max(s, axis=0, keepdims=True))
            shrink = jnp.exp2(top - new_top)
            p = jnp.exp2(s - new_top)
            total = total * shrink + jnp.sum(p, axis=0, keepdims=True)
            out.append((new_top, total, acc * shrink + weighted(values, p.astype(BF16))))
        return tuple(out)

    state = lax.fori_loop(0, i, step, tuple(state))
    result = jnp.concatenate([acc / total for _, total, acc in state], axis=1)[:head_dim].astype(BF16)
    for n in range(rows // share):
        o_ref[n] = result[:, n * share : (n + 1) * share]


def attention(gathered, w_head, share, head_dim):
    shares, _, width = gathered.shape
    group = math.gcd(4, shares)
    part = 2 * share if group % 2 == 0 else share
    tokens = shares * share
    flops = 2 * tokens * width * 3 * LANES + 4 * tokens * tokens * LANES
    return pl.pallas_call(
        functools.partial(attention_kernel, 1.0 / math.sqrt(head_dim), part, share, head_dim),
        grid=(shares // group,),
        out_shape=jax.ShapeDtypeStruct((shares, head_dim, share), BF16),
        in_specs=[pl.BlockSpec((group, share, width), lambda i: (i, 0, 0)), pl.BlockSpec((width, 3 * LANES), lambda i: (0, 0))],
        out_specs=pl.BlockSpec((group, head_dim, share), lambda i: (i, 0, 0)),
        scratch_shapes=[pltpu.VMEM((tokens, LANES), BF16), pltpu.VMEM((tokens, LANES), BF16)],
        cost_estimate=pl.CostEstimate(flops=flops, bytes_accessed=2 * tokens * width, transcendentals=tokens * tokens // 2),
        compiler_params=pltpu.CompilerParams(dimension_semantics=("arbitrary",), vmem_limit_bytes=60 * 1024 * 1024),
        name="attention",
    )(gathered, w_head)


def mlp_kernel(parts, *refs):
    rows_ref, weights = refs[0], refs[1 : 1 + 3 * parts]
    own_ref, other_ref, up_all, down_all, act_all, turned, sems = refs[1 + 3 * parts :]
    half = own_ref.shape[0]
    units = up_all.shape[0] // parts

    def fetch(m, which):
        to = (up_all, down_all)[which].at[pl.ds(m * units, units)]
        return pltpu.make_async_copy(weights[3 * m + 2 * which], to, sems.at[which, m])

    for which in range(2):
        for m in range(parts):
            fetch(m, which).start()
    turned[...] = rows_ref[...].T
    for m in range(parts):
        fetch(m, 0).wait()
        here = slice(m * units, (m + 1) * units)
        pre_act = jnp.dot(up_all[here, :], turned[...], preferred_element_type=F32) + weights[3 * m + 1][...].T
        act_all[here, :] = jax.nn.gelu(pre_act, approximate=True).astype(BF16)
    for m in range(parts):
        fetch(m, 1).wait()
    for n, out_ref in enumerate((own_ref, other_ref)):
        act = act_all[:, n * half : (n + 1) * half]
        out_ref[...] = lax.dot_general(act, down_all[...], (((0,), (0,)), ((), ())), preferred_element_type=F32)


def mlp(both, weights):
    rows, width = both.shape
    units, parts = weights[0][0].shape[0], len(weights)
    whole, far = pl.BlockSpec(memory_space=pltpu.VMEM), pl.BlockSpec(memory_space=pl.ANY)
    return pl.pallas_call(
        functools.partial(mlp_kernel, parts),
        out_shape=[jax.ShapeDtypeStruct((rows // 2, width), F32)] * 2,
        in_specs=[whole] + [far, whole, far] * parts,
        out_specs=[whole, whole],
        scratch_shapes=[
            pltpu.VMEM((parts * units, width), BF16),
            pltpu.VMEM((parts * units, width), BF16),
            pltpu.VMEM((parts * units, rows), BF16),
            pltpu.VMEM((width, rows), BF16),
            pltpu.SemaphoreType.DMA((2, parts)),
        ],
        cost_estimate=pl.CostEstimate(flops=4 * rows * width * units * parts, bytes_accessed=4 * units * width * parts, transcendentals=rows * units * parts),
        compiler_params=pltpu.CompilerParams(vmem_limit_bytes=60 * 1024 * 1024),
        name="mlp",
    )(both, *[x for up, bias, down in weights for x in (up, bias[None], down)])


def solution(mesh):
    tp_size, dp_size = mesh.shape["tp"], mesh.shape["dp"]
    bits = [1 << n for n in range(dp_size.bit_length() - 1)]

    def spread(block, order):
        held = {0: block}
        for bit in order:
            pairs = [(d, d ^ bit) for d in range(dp_size)]
            held.update({off ^ bit: lax.ppermute(b, "dp", pairs) for off, b in list(held.items())})
        return held

    def partner(x):
        return lax.ppermute(x, "tp", [(t, t ^ 1) for t in range(tp_size)])

    def forward(x_local, ln1_gain, ln1_bias, ln2_gain, ln2_bias, w_qkv, w_out, b_out, w_up, b_up, w_down, b_down):
        layers, width, hidden = w_up.shape
        share, head_dim = x_local.shape[1], w_out.shape[2]
        mine = lax.axis_index("dp")
        core = lax.rem(lax.axis_index("tp"), 2)
        part = hidden // dp_size

        def of_my_core(x):
            x = x.reshape(tp_size // 2, 2, *x.shape[1:])
            return lax.dynamic_index_in_dim(x, core, 1, keepdims=False)

        b_up_all = lax.all_gather(b_up, "tp", axis=0)
        x_local, b_up_all = lax.optimization_barrier((x_local, b_up_all))
        b_up_all = of_my_core(b_up_all).reshape(tp_size // 2, layers, dp_size, part)

        def stacked(layer):
            up = lax.dynamic_slice(w_up, (layer, 0, mine * part), (1, width, part))[0].T
            down = lax.dynamic_slice(w_down, (layer, mine * part, 0), (1, part, width))[0]
            return jnp.concatenate([up, down], 0)

        def mlp_weights(layer, to_pair, after):
            pair = lax.all_gather(to_pair, "tp", axis=0)
            if after is not None:
                pair, _ = lax.optimization_barrier((pair, after))
            pair = pair.reshape(tp_size // 2, 2, 2, part, width)
            up, down = (lax.dynamic_slice(pair, (0, core, n, 0, 0), (tp_size // 2, 1, 1, part, width)).reshape(-1, width) for n in range(2))
            ups, downs = spread(up, bits), spread(down, bits[::-1])
            out = []
            for off in range(dp_size):
                bias = lax.dynamic_index_in_dim(b_up_all[:, layer], mine ^ off, 1, keepdims=False).reshape(-1)
                out.append((ups[off], bias, downs[off]))
            return out

        weights = mlp_weights(0, stacked(0), None)
        resid = x_local[0].astype(F32)
        for layer in range(layers):
            w_head = jnp.pad(w_qkv[layer][:, :, 0], ((0, 0), (0, 0), (0, LANES - head_dim))).reshape(width, 3 * LANES)
            normed = layer_norm(resid, ln1_gain[layer], ln1_bias[layer])
            if layer == 0:
                normed, to_pair = lax.optimization_barrier((normed, stacked(1)))
            to_send = jnp.concatenate([normed, w_out[layer][0]], 0) if layer == 0 else normed
            gathered = lax.all_gather(to_send, "tp", axis=0)
            gathered, _ = lax.optimization_barrier((gathered, [w[::2] for w in weights[:1]]))
            heads = attention(gathered, w_head, share, head_dim)
            heads = lax.all_to_all(heads, "tp", 0, 0, tiled=True).reshape(-1, share)
            if layer == 0:
                w_out_all = gathered[:, share:].reshape(-1, width)
            else:
                w_out_all = lax.all_gather(w_out[layer][0], "tp", axis=0, tiled=True)
            attn = lax.dot_general(heads, w_out_all, (((0,), (0,)), ((), ())), preferred_element_type=F32)
            resid = resid + (attn + b_out[layer])
            normed_mlp = layer_norm(resid, ln2_gain[layer], ln2_bias[layer])
            both = jnp.concatenate([normed_mlp, partner(normed_mlp)], 0)
            ahead = mlp_weights(layer + 1, to_pair, normed_mlp) if layer + 1 < layers else None
            own, other = mlp(both, weights)
            summed = own + partner(other)
            resid = resid + (summed + b_down[layer])
            weights = ahead
        return resid.astype(BF16)[None]

    rows_spec = P("dp", "tp", None)
    in_specs = (rows_spec, P(), P(), P(), P(), P(None, None, None, "tp", None), P(None, "tp", None, None), P(), P(None, None, "tp"), P(None, "tp"), P(None, "tp", None), P())
    return jax.shard_map(forward, mesh=mesh, in_specs=in_specs, out_specs=rows_spec, check_vma=False)
```

```python
import functools
import math
import jax
import jax.numpy as jnp
from jax import lax
from jax.experimental import pallas as pl
from jax.experimental.pallas import tpu as pltpu
from jax.sharding import PartitionSpec as P

BF16, F32 = jnp.bfloat16, jnp.float32
LANES = 128


def layer_norm(resid, gain, shift):
    row_mean = jnp.mean(resid, axis=-1, keepdims=True)
    centered = resid - row_mean
    variance = jnp.mean(centered * centered, axis=-1, keepdims=True)
    return (centered * lax.rsqrt(variance + 1e-5) * gain + shift).astype(BF16)


def attention_kernel(scale, part, share, head_dim, h_ref, w_ref, o_ref, k_scr, v_scr):
    i = pl.program_id(0)
    rows = k_scr.shape[0] // pl.num_programs(0)
    here = pl.ds(pl.multiple_of(i * rows, rows), rows)
    hidden = h_ref[...].reshape(rows, h_ref.shape[-1])
    qkv = lax.dot_general(w_ref[...], hidden, (((1,), (1,)), ((), ())), preferred_element_type=F32).astype(BF16)
    q, k, v = (qkv[n * head_dim : (n + 1) * head_dim] for n in range(3))
    k = k.T
    k_scr[here, :] = k
    v_scr[:, here] = v
    to_exp2 = scale * math.log2(math.e)
    queries = [q[:, n * part : (n + 1) * part] for n in range(rows // part)]

    def scores(keys, query):
        return jnp.dot(keys, query, preferred_element_type=F32) * to_exp2

    def weighted(values, probs):
        return jnp.dot(values, probs.astype(BF16), preferred_element_type=F32)

    state = []
    for n, query in enumerate(queries):
        seen = (n + 1) * part
        s = scores(k[:seen], query)
        key_at = lax.broadcasted_iota(jnp.int32, s.shape, 0)
        query_at = lax.broadcasted_iota(jnp.int32, s.shape, 1) + n * part
        s = jnp.where(key_at <= query_at, s, -jnp.inf)
        top = jnp.max(s, axis=0, keepdims=True)
        p = jnp.exp2(s - top)
        state.append((top, jnp.sum(p, axis=0, keepdims=True), weighted(v[:, :seen], p)))

    def step(j, state):
        there = pl.ds(pl.multiple_of(j * rows, rows), rows)
        keys, values = k_scr[there, :], v_scr[:, there]
        blocks = [scores(keys, query) for query in queries]
        out = []
        for s, (top, total, acc) in zip(blocks, state):
            new_top = jnp.maximum(top, jnp.max(s, axis=0, keepdims=True))
            shrink = jnp.exp2(top - new_top)
            p = jnp.exp2(s - new_top)
            total = total * shrink + jnp.sum(p, axis=0, keepdims=True)
            out.append((new_top, total, acc * shrink + weighted(values, p)))
        return tuple(out)

    state = lax.fori_loop(0, i, step, tuple(state))
    result = jnp.concatenate([acc / total for _, total, acc in state], axis=1).astype(BF16)
    for n in range(rows // share):
        o_ref[n] = result[:, n * share : (n + 1) * share]


def attention(gathered, w_head, share, head_dim):
    shares, _, width = gathered.shape
    group = math.gcd(4, shares)
    part = 2 * share if group % 2 == 0 else share
    tokens = shares * share
    flops = 6 * tokens * width * head_dim + 4 * tokens * tokens * head_dim
    return pl.pallas_call(
        functools.partial(attention_kernel, 1.0 / math.sqrt(head_dim), part, share, head_dim),
        grid=(shares // group,),
        out_shape=jax.ShapeDtypeStruct((shares, head_dim, share), BF16),
        in_specs=[pl.BlockSpec((group, share, width), lambda i: (i, 0, 0)), pl.BlockSpec((3 * head_dim, width), lambda i: (0, 0))],
        out_specs=pl.BlockSpec((group, head_dim, share), lambda i: (i, 0, 0)),
        scratch_shapes=[pltpu.VMEM((tokens, head_dim), BF16), pltpu.VMEM((head_dim, tokens), BF16)],
        cost_estimate=pl.CostEstimate(flops=flops, bytes_accessed=2 * tokens * width, transcendentals=tokens * tokens // 2),
        compiler_params=pltpu.CompilerParams(dimension_semantics=("arbitrary",), vmem_limit_bytes=60 * 1024 * 1024),
        name="attention",
    )(gathered, w_head)


def mlp_kernel(parts, rows_ref, bias_ref, *refs):
    weights = refs[: 2 * parts]
    own_ref, other_ref, up_all, down_all, act_all, turned, sems = refs[2 * parts :]
    half, width = own_ref.shape
    units = up_all.shape[0] // parts

    def part_of(m):
        return pl.ds(pl.multiple_of(m * units, 16), units)

    def fetch(m, which, source):
        return pltpu.make_async_copy(weights[2 * source + which], (up_all, down_all)[which].at[part_of(m)], sems.at[which, m])

    for which in range(2):
        for m in range(parts):
            fetch(m, which, m).start()
    turned[...] = rows_ref[...].T

    def lift(m, carry):
        fetch(m, 0, 0).wait()
        here = part_of(m)
        pre_act = jnp.dot(up_all[here, :], turned[...], preferred_element_type=F32) + bias_ref[m].T
        act_all[here, :] = jax.nn.gelu(pre_act, approximate=True).astype(BF16)
        return carry

    lax.fori_loop(0, parts, lift, 0)
    for m in range(parts):
        fetch(m, 1, m).wait()
    tile = math.gcd(width, 4 * LANES)

    def lower(n, carry):
        columns = pl.ds(pl.multiple_of(n * tile, tile), tile)
        result = lax.dot_general(act_all[...], down_all[:, columns], (((0,), (0,)), ((), ())), preferred_element_type=F32)
        own_ref[:, columns] = result[:half]
        other_ref[:, columns] = result[half:]
        return carry

    lax.fori_loop(0, width // tile, lower, 0)


def mlp(both, weights):
    rows, width = both.shape
    units, parts = weights[0][0].shape[0], len(weights)
    whole, far = pl.BlockSpec(memory_space=pltpu.VMEM), pl.BlockSpec(memory_space=pl.ANY)
    bias = jnp.stack([bias[None] for _, bias, _ in weights])
    return pl.pallas_call(
        functools.partial(mlp_kernel, parts),
        out_shape=[jax.ShapeDtypeStruct((rows // 2, width), F32)] * 2,
        in_specs=[whole] * 2 + [far] * (2 * parts),
        out_specs=[whole, whole],
        scratch_shapes=[
            pltpu.VMEM((parts * units, width), BF16),
            pltpu.VMEM((parts * units, width), BF16),
            pltpu.VMEM((parts * units, rows), BF16),
            pltpu.VMEM((width, rows), BF16),
            pltpu.SemaphoreType.DMA((2, parts)),
        ],
        cost_estimate=pl.CostEstimate(flops=4 * rows * width * units * parts, bytes_accessed=4 * units * width * parts, transcendentals=rows * units * parts),
        compiler_params=pltpu.CompilerParams(vmem_limit_bytes=60 * 1024 * 1024),
        name="mlp",
    )(both, bias, *[x for up, _, down in weights for x in (up, down)])


def solution(mesh):
    tp_size, dp_size = mesh.shape["tp"], mesh.shape["dp"]
    bits = [1 << n for n in range(dp_size.bit_length() - 1)]

    def spread(block, order):
        held = {0: block}
        for bit in order:
            pairs = [(d, d ^ bit) for d in range(dp_size)]
            held.update({off ^ bit: lax.ppermute(b, "dp", pairs) for off, b in list(held.items())})
        return held

    def partner(x):
        return lax.ppermute(x, "tp", [(t, t ^ 1) for t in range(tp_size)])

    def forward(x_local, ln1_gain, ln1_bias, ln2_gain, ln2_bias, w_qkv, w_out, b_out, w_up, b_up, w_down, b_down):
        layers, width, hidden = w_up.shape
        share, head_dim = x_local.shape[1], w_out.shape[2]
        mine = lax.axis_index("dp")
        core = lax.rem(lax.axis_index("tp"), 2)
        part = hidden // dp_size

        def of_my_core(x):
            x = x.reshape(tp_size // 2, 2, *x.shape[1:])
            return lax.dynamic_index_in_dim(x, core, 1, keepdims=False)

        b_up_all = lax.all_gather(b_up, "tp", axis=0)
        x_local, b_up_all = lax.optimization_barrier((x_local, b_up_all))
        b_up_all = of_my_core(b_up_all).reshape(tp_size // 2, layers, dp_size, part)

        def stacked(layer):
            up = lax.dynamic_slice(w_up, (layer, 0, mine * part), (1, width, part))[0].T
            down = lax.dynamic_slice(w_down, (layer, mine * part, 0), (1, part, width))[0]
            return jnp.concatenate([up, down], 0)

        def mlp_weights(layer, to_pair, after):
            pair = lax.all_gather(to_pair, "tp", axis=0)
            if after is not None:
                pair, _ = lax.optimization_barrier((pair, after))
            pair = pair.reshape(tp_size // 2, 2, 2, part, width)
            up, down = (lax.dynamic_slice(pair, (0, core, n, 0, 0), (tp_size // 2, 1, 1, part, width)).reshape(-1, width) for n in range(2))
            ups, downs = spread(up, bits), spread(down, bits[::-1])
            out = []
            for off in range(dp_size):
                bias = lax.dynamic_index_in_dim(b_up_all[:, layer], mine ^ off, 1, keepdims=False).reshape(-1)
                out.append((ups[off], bias, downs[off]))
            return out

        weights = mlp_weights(0, stacked(0), None)
        resid = x_local[0].astype(F32)
        for layer in range(layers):
            w_head = w_qkv[layer][:, :, 0].reshape(width, 3 * head_dim).T
            normed = layer_norm(resid, ln1_gain[layer], ln1_bias[layer])
            if layer == 0:
                normed, to_pair = lax.optimization_barrier((normed, stacked(1)))
            to_send = jnp.concatenate([normed, w_out[layer][0]], 0) if layer == 0 else normed
            gathered = lax.all_gather(to_send, "tp", axis=0)
            gathered, _ = lax.optimization_barrier((gathered, [w[::2] for w in weights[:1]]))
            heads = attention(gathered, w_head, share, head_dim)
            heads = lax.all_to_all(heads, "tp", 0, 0, tiled=True).reshape(-1, share)
            if layer == 0:
                w_out_all = gathered[:, share:].reshape(-1, width)
            else:
                w_out_all = lax.all_gather(w_out[layer][0], "tp", axis=0, tiled=True)
            attn = lax.dot_general(heads, w_out_all, (((0,), (0,)), ((), ())), preferred_element_type=F32)
            resid = resid + (attn + b_out[layer])
            normed_mlp = layer_norm(resid, ln2_gain[layer], ln2_bias[layer])
            both = jnp.concatenate([normed_mlp, partner(normed_mlp)], 0)
            ahead = mlp_weights(layer + 1, to_pair, normed_mlp) if layer + 1 < layers else None
            own, other = mlp(both, weights)
            summed = own + partner(other)
            resid = resid + (summed + b_down[layer])
            weights = ahead
        return resid.astype(BF16)[None]

    rows_spec = P("dp", "tp", None)
    in_specs = (rows_spec, P(), P(), P(), P(), P(None, None, None, "tp", None), P(None, "tp", None, None), P(), P(None, None, "tp"), P(None, "tp"), P(None, "tp", None), P())
    return jax.shard_map(forward, mesh=mesh, in_specs=in_specs, out_specs=rows_spec, check_vma=False)
```

```python
import functools
import math
import jax
import jax.numpy as jnp
from jax import lax
from jax.experimental import pallas as pl
from jax.experimental.pallas import tpu as pltpu
from jax.sharding import PartitionSpec as P

BF16, F32 = jnp.bfloat16, jnp.float32
LANES = 128


def layer_norm(resid, gain, shift):
    row_mean = jnp.mean(resid, axis=-1, keepdims=True)
    centered = resid - row_mean
    variance = jnp.mean(centered * centered, axis=-1, keepdims=True)
    return (centered * lax.rsqrt(variance + 1e-5) * gain + shift).astype(BF16)


def attention_kernel(scale, part, share, head_dim, h_ref, w_ref, o_ref, k_scr, v_scr):
    i = pl.program_id(0)
    rows = k_scr.shape[0] // pl.num_programs(0)
    here = pl.ds(pl.multiple_of(i * rows, rows), rows)
    hidden = h_ref[...].reshape(rows, h_ref.shape[-1])
    qkv = lax.dot_general(w_ref[...], hidden, (((1,), (1,)), ((), ())), preferred_element_type=F32).astype(BF16)
    q, k, v = (qkv[n * head_dim : (n + 1) * head_dim] for n in range(3))
    k = k.T
    k_scr[here, :] = k
    v_scr[:, here] = v
    to_exp2 = scale * math.log2(math.e)
    queries = [q[:, n * part : (n + 1) * part] for n in range(rows // part)]

    def scores(keys, query):
        return jnp.dot(keys, query, preferred_element_type=F32) * to_exp2

    def weighted(values, probs):
        return jnp.dot(values, probs.astype(BF16), preferred_element_type=F32)

    state = []
    for n, query in enumerate(queries):
        seen = (n + 1) * part
        s = scores(k[:seen], query)
        key_at = lax.broadcasted_iota(jnp.int32, s.shape, 0)
        query_at = lax.broadcasted_iota(jnp.int32, s.shape, 1) + n * part
        s = jnp.where(key_at <= query_at, s, -jnp.inf)
        top = jnp.max(s, axis=0, keepdims=True)
        p = jnp.exp2(s - top)
        state.append((top, jnp.sum(p, axis=0, keepdims=True), weighted(v[:, :seen], p)))

    def step(j, state):
        there = pl.ds(pl.multiple_of(j * rows, rows), rows)
        keys, values = k_scr[there, :], v_scr[:, there]
        blocks = [scores(keys, query) for query in queries]
        out = []
        for s, (top, total, acc) in zip(blocks, state):
            new_top = jnp.maximum(top, jnp.max(s, axis=0, keepdims=True))
            shrink = jnp.exp2(top - new_top)
            p = jnp.exp2(s - new_top)
            total = total * shrink + jnp.sum(p, axis=0, keepdims=True)
            out.append((new_top, total, acc * shrink + weighted(values, p)))
        return tuple(out)

    state = lax.fori_loop(0, i, step, tuple(state))
    result = jnp.concatenate([acc / total for _, total, acc in state], axis=1).astype(BF16)
    for n in range(rows // share):
        o_ref[n] = result[:, n * share : (n + 1) * share]


def attention(gathered, w_head, share, head_dim):
    shares, _, width = gathered.shape
    group = math.gcd(4, shares)
    part = 2 * share if group % 2 == 0 else share
    tokens = shares * share
    flops = 6 * tokens * width * head_dim + 4 * tokens * tokens * head_dim
    return pl.pallas_call(
        functools.partial(attention_kernel, 1.0 / math.sqrt(head_dim), part, share, head_dim),
        grid=(shares // group,),
        out_shape=jax.ShapeDtypeStruct((shares, head_dim, share), BF16),
        in_specs=[pl.BlockSpec((group, share, width), lambda i: (i, 0, 0)), pl.BlockSpec((3 * head_dim, width), lambda i: (0, 0))],
        out_specs=pl.BlockSpec((group, head_dim, share), lambda i: (i, 0, 0)),
        scratch_shapes=[pltpu.VMEM((tokens, head_dim), BF16), pltpu.VMEM((head_dim, tokens), BF16)],
        cost_estimate=pl.CostEstimate(flops=flops, bytes_accessed=2 * tokens * width, transcendentals=tokens * tokens // 2),
        compiler_params=pltpu.CompilerParams(dimension_semantics=("arbitrary",), vmem_limit_bytes=60 * 1024 * 1024),
        name="attention",
    )(gathered, w_head)


def mlp_kernel(parts, rows_ref, bias_ref, *refs):
    weights = refs[: 2 * parts]
    own_ref, other_ref, up_all, down_all, act_all, turned, sems = refs[2 * parts :]
    half, width = own_ref.shape
    units = up_all.shape[0] // parts

    def part_of(m):
        return pl.ds(pl.multiple_of(m * units, 16), units)

    def fetch(m, which, source):
        return pltpu.make_async_copy(weights[2 * source + which], (up_all, down_all)[which].at[part_of(m)], sems.at[which, m])

    for which in range(2):
        for m in range(parts):
            fetch(m, which, m).start()
    turned[...] = rows_ref[...].T

    def lift(m, carry):
        fetch(m, 0, 0).wait()
        here = part_of(m)
        pre_act = jnp.dot(up_all[here, :], turned[...], preferred_element_type=F32) + bias_ref[m].T
        act_all[here, :] = jax.nn.gelu(pre_act, approximate=True).astype(BF16)
        return carry

    lax.fori_loop(0, parts, lift, 0)
    for m in range(parts):
        fetch(m, 1, m).wait()
    tile = math.gcd(width, 4 * LANES)

    def lower(n, carry):
        columns = pl.ds(pl.multiple_of(n * tile, tile), tile)
        result = lax.dot_general(act_all[...], down_all[:, columns], (((0,), (0,)), ((), ())), preferred_element_type=F32)
        own_ref[:, columns] = result[:half]
        other_ref[:, columns] = result[half:]
        return carry

    lax.fori_loop(0, width // tile, lower, 0)


def mlp(both, weights):
    rows, width = both.shape
    units, parts = weights[0][0].shape[0], len(weights)
    whole, far = pl.BlockSpec(memory_space=pltpu.VMEM), pl.BlockSpec(memory_space=pl.ANY)
    bias = jnp.stack([bias[None] for _, bias, _ in weights])
    return pl.pallas_call(
        functools.partial(mlp_kernel, parts),
        out_shape=[jax.ShapeDtypeStruct((rows // 2, width), F32)] * 2,
        in_specs=[whole] * 2 + [far] * (2 * parts),
        out_specs=[whole, whole],
        scratch_shapes=[
            pltpu.VMEM((parts * units, width), BF16),
            pltpu.VMEM((parts * units, width), BF16),
            pltpu.VMEM((parts * units, rows), BF16),
            pltpu.VMEM((width, rows), BF16),
            pltpu.SemaphoreType.DMA((2, parts)),
        ],
        cost_estimate=pl.CostEstimate(flops=4 * rows * width * units * parts, bytes_accessed=4 * units * width * parts, transcendentals=rows * units * parts),
        compiler_params=pltpu.CompilerParams(vmem_limit_bytes=60 * 1024 * 1024),
        name="mlp",
    )(both, bias, *[x for up, _, down in weights for x in (up, down)])


def lift_kernel(parts, rows_ref, bias_ref, *refs):
    weights, (act_ref, up_all, turned, sems) = refs[:parts], refs[parts:]
    units = up_all.shape[0] // parts

    def fetch(m, source):
        return pltpu.make_async_copy(weights[source], up_all.at[pl.ds(pl.multiple_of(m * units, 16), units)], sems.at[m])

    for m in range(parts):
        fetch(m, m).start()
    turned[...] = rows_ref[...].T

    def lift(m, carry):
        fetch(m, 0).wait()
        here = pl.ds(pl.multiple_of(m * units, 16), units)
        pre_act = jnp.dot(up_all[here, :], turned[...], preferred_element_type=F32) + bias_ref[m].T
        act_ref[here, :] = jax.nn.gelu(pre_act, approximate=True).astype(BF16)
        return carry

    lax.fori_loop(0, parts, lift, 0)


def lower_kernel(parts, act_ref, *refs):
    weights, (own_ref, other_ref, down_all, sems) = refs[:parts], refs[parts:]
    half, width = own_ref.shape
    units = down_all.shape[0] // parts
    tile = math.gcd(width, 4 * LANES)

    def fetch(n, m):
        columns = pl.ds(pl.multiple_of(n * tile, tile), tile)
        return pltpu.make_async_copy(weights[m].at[:, columns], down_all.at[pl.ds(m * units, units), columns], sems.at[n, m])

    for n in range(width // tile):
        for m in range(parts):
            fetch(n, m).start()

    def lower(n, carry):
        for m in range(parts):
            fetch(n, m).wait()
        columns = pl.ds(pl.multiple_of(n * tile, tile), tile)
        result = lax.dot_general(act_ref[...], down_all[:, columns], (((0,), (0,)), ((), ())), preferred_element_type=F32)
        own_ref[:, columns] = result[:half]
        other_ref[:, columns] = result[half:]
        return carry

    lax.fori_loop(0, width // tile, lower, 0)


def mlp_lift(both, weights):
    rows, width = both.shape
    units, parts = weights[0][0].shape[0], len(weights)
    whole, far = pl.BlockSpec(memory_space=pltpu.VMEM), pl.BlockSpec(memory_space=pl.ANY)
    return pl.pallas_call(
        functools.partial(lift_kernel, parts),
        out_shape=jax.ShapeDtypeStruct((parts * units, rows), BF16),
        in_specs=[whole] * 2 + [far] * parts,
        out_specs=whole,
        scratch_shapes=[pltpu.VMEM((parts * units, width), BF16), pltpu.VMEM((width, rows), BF16), pltpu.SemaphoreType.DMA((parts,))],
        cost_estimate=pl.CostEstimate(flops=2 * rows * width * units * parts, bytes_accessed=2 * units * width * parts, transcendentals=rows * units * parts),
        compiler_params=pltpu.CompilerParams(vmem_limit_bytes=60 * 1024 * 1024),
        name="mlp_lift",
    )(both, jnp.stack([bias[None] for _, bias, _ in weights]), *[up for up, _, _ in weights])


def mlp_lower(act, weights):
    rows = act.shape[1]
    (units, width), parts = weights[0][2].shape, len(weights)
    whole, far = pl.BlockSpec(memory_space=pltpu.VMEM), pl.BlockSpec(memory_space=pl.ANY)
    return pl.pallas_call(
        functools.partial(lower_kernel, parts),
        out_shape=[jax.ShapeDtypeStruct((rows // 2, width), F32)] * 2,
        in_specs=[whole] + [far] * parts,
        out_specs=[whole, whole],
        scratch_shapes=[pltpu.VMEM((parts * units, width), BF16), pltpu.SemaphoreType.DMA((width // math.gcd(width, 4 * LANES), parts))],
        cost_estimate=pl.CostEstimate(flops=2 * rows * width * units * parts, bytes_accessed=2 * units * width * parts, transcendentals=0),
        compiler_params=pltpu.CompilerParams(vmem_limit_bytes=60 * 1024 * 1024),
        name="mlp_lower",
    )(act, *[down for _, _, down in weights])


def solution(mesh):
    tp_size, dp_size = mesh.shape["tp"], mesh.shape["dp"]
    bits = [1 << n for n in range(dp_size.bit_length() - 1)]

    def spread(block, order):
        held = {0: block}
        for bit in order:
            pairs = [(d, d ^ bit) for d in range(dp_size)]
            held.update({off ^ bit: lax.ppermute(b, "dp", pairs) for off, b in list(held.items())})
        return held

    def partner(x):
        return lax.ppermute(x, "tp", [(t, t ^ 1) for t in range(tp_size)])

    def forward(x_local, ln1_gain, ln1_bias, ln2_gain, ln2_bias, w_qkv, w_out, b_out, w_up, b_up, w_down, b_down):
        layers, width, hidden = w_up.shape
        share, head_dim = x_local.shape[1], w_out.shape[2]
        mine = lax.axis_index("dp")
        core = lax.rem(lax.axis_index("tp"), 2)
        part = hidden // dp_size

        def of_my_core(x):
            x = x.reshape(tp_size // 2, 2, *x.shape[1:])
            return lax.dynamic_index_in_dim(x, core, 1, keepdims=False)

        b_up_all = lax.all_gather(b_up, "tp", axis=0)
        x_local, b_up_all = lax.optimization_barrier((x_local, b_up_all))
        b_up_all = of_my_core(b_up_all).reshape(tp_size // 2, layers, dp_size, part)

        def stacked(layer):
            up = lax.dynamic_slice(w_up, (layer, 0, mine * part), (1, width, part))[0].T
            down = lax.dynamic_slice(w_down, (layer, mine * part, 0), (1, part, width))[0]
            return jnp.concatenate([up, down], 0)

        def mlp_weights(layer, to_pair, after):
            pair = lax.all_gather(to_pair, "tp", axis=0)
            if after is not None:
                pair, _ = lax.optimization_barrier((pair, after))
            pair = pair.reshape(tp_size // 2, 2, 2, part, width)
            up, down = (lax.dynamic_slice(pair, (0, core, n, 0, 0), (tp_size // 2, 1, 1, part, width)).reshape(-1, width) for n in range(2))
            ups, downs = spread(up, bits), spread(down, bits[::-1])
            out = []
            for off in range(dp_size):
                bias = lax.dynamic_index_in_dim(b_up_all[:, layer], mine ^ off, 1, keepdims=False).reshape(-1)
                out.append((ups[off], bias, downs[off]))
            return out

        weights = mlp_weights(0, stacked(0), None)
        resid = x_local[0].astype(F32)
        for layer in range(layers):
            w_head = w_qkv[layer][:, :, 0].reshape(width, 3 * head_dim).T
            normed = layer_norm(resid, ln1_gain[layer], ln1_bias[layer])
            if layer == 0:
                normed, to_pair = lax.optimization_barrier((normed, stacked(1)))
            to_send = jnp.concatenate([normed, w_out[layer][0]], 0) if layer == 0 else normed
            gathered = lax.all_gather(to_send, "tp", axis=0)
            gathered, _ = lax.optimization_barrier((gathered, [w[::2] for w in weights[:1]]))
            heads = attention(gathered, w_head, share, head_dim)
            heads = lax.all_to_all(heads, "tp", 0, 0, tiled=True).reshape(-1, share)
            if layer == 0:
                w_out_all = gathered[:, share:].reshape(-1, width)
            else:
                w_out_all = lax.all_gather(w_out[layer][0], "tp", axis=0, tiled=True)
            attn = lax.dot_general(heads, w_out_all, (((0,), (0,)), ((), ())), preferred_element_type=F32)
            resid = resid + (attn + b_out[layer])
            normed_mlp = layer_norm(resid, ln2_gain[layer], ln2_bias[layer])
            both = jnp.concatenate([normed_mlp, partner(normed_mlp)], 0)
            ahead = None
            if layer + 1 < layers:
                act = mlp_lift(both, weights)
                ahead = mlp_weights(layer + 1, to_pair, act)
                own, other = mlp_lower(act, weights)
            else:
                own, other = mlp(both, weights)
            summed = own + partner(other)
            resid = resid + (summed + b_down[layer])
            weights = ahead
        return resid.astype(BF16)[None]

    rows_spec = P("dp", "tp", None)
    in_specs = (rows_spec, P(), P(), P(), P(), P(None, None, None, "tp", None), P(None, "tp", None, None), P(), P(None, None, "tp"), P(None, "tp"), P(None, "tp", None), P())
    return jax.shard_map(forward, mesh=mesh, in_specs=in_specs, out_specs=rows_spec, check_vma=False)
```
